768 devices in a mesh: gx: 48 (over x, z), gy: 4 (over y_hi, core), gz: 4 (over y_lo).
Axes of the slice: x: 4, y: 8 (y_hi: 2, y_lo: 4; y = y_hi * 4 + y_lo), z: 12, core: 2. Of those that a mesh axis runs over, the one named last changes fastest.
Arguments:
- composition: float32 [106, 96, 16, 512], P(None, 'gx', 'gy', 'gz'), may hold values from -6 to 6
- inv_temp: bfloat16 [96, 16, 512], P('gx', 'gy', 'gz'), may hold values from 0.3984375 to 1.59375
- diffusivity: float32 [106], replicated, may hold values from 0.01 to 0.1
- reactant_orders: bfloat16 [420, 106], replicated, may hold values from 0 to 0.019897461
- net_stoich: bfloat16 [106, 420], replicated, may hold values from -0.3125 to 0.3125
- log_rate: float32 [420], replicated, may hold values from -1 to 1
- activation: float32 [420], replicated, may hold values from 0.5 to 3
- hot_blocks: int32 [48, 4, 4, 8], P('gx', 'gy', 'gz'), may hold values from 0 to 7, as said below
- hot_counts: int32 [48, 4, 4], P('gx', 'gy', 'gz'), may hold values from 1 to 8, as said below
Outputs:
- composition_next: float32 [106, 96, 16, 512], P(None, 'gx', 'gy', 'gz')
The draws below stay inside these ranges and needn't reach their ends.
Inputs may be any that keep to these rules, and one draw needn't show every extreme that they name: `hot_blocks`: each device's row holds 8 distinct block numbers of that device. `hot_counts`: some device has exactly 8 hot blocks.
All inputs are finite; a program needn't handle non-finite values.
Results may differ from the reference program's by a relative error of at most 0.0015.
Values may be sent and summed in bfloat16 or wider, within the bound.
No kernel may reach another device: no remote copies, remote signals or barrier semaphores. Data moves between devices by JAX's collectives and lax.ppermute only.
A program may use at most 32 MiB of HBM per device.

```python
import math
import jax
import jax.numpy as jnp
from jax import lax

S = 106
R = 420
CZ = 128
SECTIONS = 4
CX = 2
CY = 4
HOT = 8
NX = 96
NY = 16
NZ = 512
N_GX = 48
N_GY = 4
N_GZ = 4
DEVICES = 768


def draw_hot_blocks(key, part):
    keys = jax.random.split(jax.random.fold_in(key, 11), DEVICES)

    def choose_row(row_key):
        return jax.random.permutation(row_key, CX * CY)[:HOT]
    rows = jax.vmap(choose_row)(keys)
    return rows.astype(jnp.int32).reshape(N_GX, N_GY, N_GZ, HOT)


def draw_hot_counts(key, part):
    folded = jax.random.fold_in(key, 23)
    drawn = jax.random.randint(folded, (DEVICES,), 0, HOT)
    counts = 1 + drawn * drawn // HOT
    picked = jax.random.randint(jax.random.fold_in(folded, 1), (), 0, DEVICES)
    counts = jnp.where(jnp.arange(DEVICES) == picked, HOT, counts)
    counts = jnp.minimum(counts, HOT)
    return counts.astype(jnp.int32).reshape(N_GX, N_GY, N_GZ)


def shard_levels(stream_key, dims, cuts, smallest, high):
    loudness = 1.0
    for dim, shards_of in cuts:
        heights = jax.random.uniform(jax.random.fold_in(jax.random.fold_in(stream_key, 6), dim), (shards_of,), jnp.float32, smallest / len(cuts), high / len(cuts))
        loudness = loudness * jnp.repeat(jnp.exp(heights), dims[dim] // shards_of).reshape((-1,) + (1,) * (len(dims) - 1 - dim))
    return loudness


def bell_draw(key, shape, width, bound, shards=(), kind=jnp.bfloat16):
    values = jax.random.normal(key, shape, jnp.float32) * width
    if len(shards) > 0:
        values = shard_levels(key, shape, shards, -0.22, 0.18) * values
    return jnp.clip(values, min=-bound, max=bound).astype(kind)


def setup_inputs(seed: int = 0) -> dict:
    splits = jax.random.split(jax.random.key(seed), 10)
    return {
        "composition": bell_draw(splits[0], (S, NX, NY, NZ), 1.0, 6.0, ((1, 48), (2, 4), (3, 4)), jnp.float32),
        "inv_temp": jnp.clip(jnp.exp(math.log(1.59375) - 1.3862944 * jax.random.uniform(splits[1], (NX, NY, NZ), jnp.float32) ** shard_levels(splits[1], (NX, NY, NZ), ((0, 48), (1, 4), (2, 4)), -0.2, 0.2)), 0.3984375, 1.59375).astype(jnp.bfloat16),
        "diffusivity": jnp.clip(jnp.exp(jax.random.uniform(splits[2], (S,), jnp.float32, math.log(0.01), math.log(0.1))), 0.01, 0.1),
        "reactant_orders": jnp.clip(jax.random.uniform(splits[3], (R, S), jnp.float32, 0.0, 0.019897461), 0.0, 0.019897461).astype(jnp.bfloat16),
        "net_stoich": bell_draw(splits[4], (S, R), R ** -0.5, 0.3125),
        "log_rate": jnp.clip(jax.random.uniform(splits[5], (R,), jnp.float32, -1.0, 1.0), -1.0, 1.0),
        "activation": jnp.clip(jax.random.uniform(splits[6], (R,), jnp.float32, 0.5, 3.0), 0.5, 3.0),
        "hot_blocks": draw_hot_blocks(jax.random.fold_in(splits[9], 71), 0),
        "hot_counts": draw_hot_counts(jax.random.fold_in(splits[9], 71), 0),
    }


rate_step = 0.5


def fourth_order(padded, axis_number, length):
    def window(offset):
        return lax.slice_in_dim(padded, offset, offset + length, axis=axis_number)
    return (16.0 * (window(1) + window(3)) - window(0) - window(4) - 30.0 * window(2)) / 12.0


def transport(field_in, diffusivity):
    field_shape = field_in.shape
    padded = jnp.pad(field_in, ((0, 0), (2, 2), (2, 2), (2, 2)), mode="wrap")
    along_x = padded[:, :, 2:-2, 2:-2]
    along_y = padded[:, 2:-2, :, 2:-2]
    along_z = padded[:, 2:-2, 2:-2, :]
    laplace_sum = fourth_order(along_x, 1, field_shape[1]) + fourth_order(along_y, 2, field_shape[2]) + fourth_order(along_z, 3, field_shape[3])
    return field_in + diffusivity[:, None, None, None] * laplace_sum


def react_cells(columns, inverse, reactant_orders, net_stoich, log_rate, activation):
    initial = columns.astype(jnp.float32)
    current = initial
    operand = columns
    inverse_cells = inverse.astype(jnp.float32)
    for repeat in range(SECTIONS):
        logits = jnp.dot(reactant_orders, operand, preferred_element_type=jnp.float32) + log_rate[:, None] - activation[:, None] * inverse_cells[None, :]
        progress = jnp.exp(logits).astype(jnp.bfloat16)
        produced = jnp.dot(net_stoich, progress, preferred_element_type=jnp.float32)
        consumed = lax.dot_general(reactant_orders, progress, (((0,), (0,)), ((), ())), preferred_element_type=jnp.float32)
        current = current + rate_step * produced / (1.0 + rate_step * consumed)
        operand = current.astype(jnp.bfloat16)
    return (current - initial).astype(jnp.bfloat16)


def reference(composition, inv_temp, diffusivity, reactant_orders, net_stoich, log_rate, activation, hot_blocks, hot_counts):
    carried = transport(composition, diffusivity)
    device_count = N_GX * N_GY * N_GZ
    blocks_total = CX * CY
    shaped = carried.reshape(S, N_GX, CX, N_GY, CY, N_GZ, CZ).transpose(1, 3, 5, 0, 2, 4, 6).reshape(device_count, S, blocks_total, CZ)
    heat_rows = inv_temp.reshape(N_GX, CX, N_GY, CY, N_GZ, CZ).transpose(0, 2, 4, 1, 3, 5).reshape(device_count, blocks_total, CZ)
    listed_all = hot_blocks.reshape(device_count, HOT)
    counts = hot_counts.reshape(device_count)

    def one_device(packed):
        state_field, heat_block, listed, live_count = packed

        def advance(slot, state_field):
            block_index = listed[slot].astype(jnp.int32)
            column_block = lax.dynamic_slice_in_dim(state_field, block_index, 1, 1).reshape(S, CZ)
            inverse = lax.dynamic_slice_in_dim(heat_block, block_index, 1, 0).reshape(CZ)
            increment = react_cells(column_block.astype(jnp.bfloat16), inverse, reactant_orders, net_stoich, log_rate, activation)
            updated = (column_block + increment.astype(jnp.float32)).reshape(S, 1, CZ)
            return lax.dynamic_update_slice_in_dim(state_field, updated, block_index, 1)

        return lax.fori_loop(jnp.int32(0), live_count.astype(jnp.int32), advance, state_field)

    reacted = lax.map(one_device, (shaped, heat_rows, listed_all, counts))
    returned = reacted.reshape(N_GX, N_GY, N_GZ, S, CX, CY, CZ).transpose(3, 0, 4, 1, 5, 2, 6).reshape(S, N_GX * CX, N_GY * CY, N_GZ * CZ)
    return transport(returned, diffusivity)
```

```python
import functools

import jax
import jax.numpy as jnp
from jax import lax
from jax.experimental import pallas as pl
from jax.experimental.pallas import tpu as pltpu
from jax.sharding import PartitionSpec as P

SECTIONS = 4
GROUP = 4

f32, bf16 = jnp.float32, jnp.bfloat16
VMEM = pl.BlockSpec(memory_space=pltpu.VMEM)
SMEM = pl.BlockSpec(memory_space=pltpu.SMEM)
ANY = pl.BlockSpec(memory_space=pl.ANY)


def ceil_to(n, k):
    return -(-n // k) * k


def swap(x, axis, phase):
    n = lax.axis_size(axis)
    pairs = []
    for i in range(phase, n, 2):
        j = (i + 1) % n
        pairs += [(i, j), (j, i)]
    return lax.ppermute(x, axis, pairs)


def chunks(species):
    return [(s, min(16, species - s)) for s in range(0, species, 16)]


def lane_of(rows):
    return lax.broadcasted_iota(jnp.int32, (rows, 128), 1)


def pick(flag, rows):
    return jnp.full((rows, 128), flag, jnp.int32) == 0


def pack(load, species, dims, odd_y, g_ref, ya_ref, yb_ref, z_ref):
    cx, cy = dims
    for s, n in chunks(species):
        lane = lane_of(n)
        even_y = pick(odd_y, n)
        edges = jnp.zeros((n, 128), f32)
        columns = []
        for c in range(cx * cy):
            v = load(c, s, n)
            columns.append(v)
            g_ref[c, s : s + n, :] = v.astype(bf16)
            edges = jnp.where((lane >> 1) == c, pltpu.roll(v, 2 * c, 1) if c else v, edges)
            edges = jnp.where((lane >> 1) == 32 + c, pltpu.roll(v, 2 * c + 66, 1), edges)
        for x in range(cx):
            for k in range(2):
                under, over = columns[x * cy + k], columns[x * cy + cy - 2 + k]
                ya_ref[x * 2 + k, s : s + n, :] = jnp.where(even_y, over, under).astype(bf16)
                yb_ref[x * 2 + k, s : s + n, :] = jnp.where(even_y, under, over).astype(bf16)
        z_ref[s : s + n, :] = edges.astype(bf16)


def stencil_of(distance):
    reach = jnp.abs(distance)
    w = jnp.where(reach == 1, 16.0, jnp.where(reach == 2, -1.0, 0.0))
    return jnp.where(reach == 0, -90.0, w)


def transport(own_ref, store, species, dims, odd, halos, rate_ref, inner_ref, outer_ref, zt):
    cx, cy = dims
    total = cx * cy
    odd_x, odd_y, odd_z = odd
    ga_ref, gb_ref, ya_ref, yb_ref, za_ref, zb_ref = halos
    sp = own_ref.shape[1]
    v = own_ref[...].reshape(total * sp, 128)
    high = v.astype(bf16)
    low = (v - high.astype(f32)).astype(bf16)
    zt[...] = jnp.dot(jnp.concatenate([high, low], axis=1), inner_ref[...], preferred_element_type=f32).reshape(total, sp, 128)
    even_z = (lane_of(species) < 64) == pick(odd_z, species)
    edges = jnp.where(even_z, za_ref[...].astype(f32), zb_ref[...].astype(f32)).astype(bf16)
    rim = jnp.dot(edges, outer_ref[...], preferred_element_type=f32)
    for c in range(total):
        zt[c, 0:species, :] = zt[c, 0:species, :] + rim[:, c * 128 : c * 128 + 128]
    for s, n in chunks(species):
        even_x, even_y = pick(odd_x, n), pick(odd_y, n)

        def both(a, b, even):
            a, b = a.astype(f32), b.astype(f32)
            return jnp.where(even, a, b), jnp.where(even, b, a)

        rows = slice(s, s + n)
        rate = rate_ref[rows, :]
        v = [own_ref[c, rows, :] for c in range(total)]
        up, down = [], []
        for k in range(2 * cx):
            above, under = both(ya_ref[k, rows, :], yb_ref[k, rows, :], even_y)
            up.append(above)
            down.append(under)
        for y in range(cy):
            right0, left0 = both(ga_ref[y, rows, :], gb_ref[y, rows, :], even_x)
            right1, left1 = both(ga_ref[cy + y, rows, :], gb_ref[cy + y, rows, :], even_x)
            line = [left0, left1, v[y], v[cy + y], right0, right1]
            for x in range(cx):
                c = x * cy + y
                ys = down[2 * x : 2 * x + 2] + v[x * cy : x * cy + cy] + up[2 * x : 2 * x + 2]
                near = (line[x + 1] + line[x + 3]) + (ys[y + 1] + ys[y + 3])
                far = (line[x] + line[x + 4]) + (ys[y] + ys[y + 4])
                store(c, s, n, v[c] + rate * (16.0 * near - far + zt[c, rows, :]))


def parities():
    return tuple(lax.rem(lax.axis_index(a), 2) for a in ("gx", "gy", "gz"))


def pack_kernel(species, dims, odd_ref, comp_ref, own_ref, *outs):
    total = dims[0] * dims[1]

    def load(c, s, n):
        value = comp_ref[pl.ds(s * total + c, n, stride=total), :]
        own_ref[c, s : s + n, :] = value
        return value

    pack(load, species, dims, odd_ref[1], *outs)


def prepare_kernel(species, reactions, columns, *refs):
    (orders_hbm, net_hbm, log_hbm, act_hbm, diff_hbm, heat_hbm) = refs[:6]
    (first_ref, second_ref, rate_ref, inner_ref, outer_ref, heat_ref) = refs[6:12]
    tall, wide, orders, net, log, act, diff, heat, sems = refs[12:]
    moves = [
        pltpu.make_async_copy(src, dst, sems.at[k])
        for k, (src, dst) in enumerate(
            [(orders_hbm, orders), (net_hbm, net), (log_hbm, log), (act_hbm, act), (diff_hbm, diff), (heat_hbm, heat)]
        )
    ]
    for move in moves:
        move.start()
    k, lane = lax.broadcasted_iota(jnp.int32, (128, 128), 0), lane_of(128)
    inner = stencil_of(lane - k).astype(bf16)
    inner_ref[0:128, :] = inner
    inner_ref[128:256, :] = inner
    outer = stencil_of(lane - (jnp.where(k < 64, 128, -2) + (k & 1)))
    for c in range(columns):
        outer_ref[:, c * 128 : c * 128 + 128] = jnp.where(((k & 63) >> 1) == c, outer, 0.0).astype(bf16)
    wide[...] = jnp.zeros_like(wide)
    tall[...] = jnp.zeros_like(tall)
    for move in moves:
        move.wait()
    heat_ref[...] = heat[...].astype(f32)
    rp, sp = first_ref.shape
    for row, ref in ((species, log), (species + 3, act)):
        rest = ref[...]
        for k in range(3):
            part = rest.astype(bf16).astype(f32)
            wide[row + k : row + k + 1, 0:reactions] = part
            rest = rest - part
    tall[0:reactions, 0:species] = orders[...].astype(f32)
    first_ref[...] = (tall[...] + wide[...].T)[0:rp, 0:sp].astype(bf16)
    second_ref[sp : 2 * sp, :] = (0.5 * tall[...]).T[0:sp, 0:rp].astype(bf16)
    tall[0:reactions, 0:species] = 0.5 * net[...].astype(f32)
    second_ref[0:sp, :] = tall[...].T[0:sp, 0:rp].astype(bf16)
    wide[0:1, 0:species] = diff[...] * (1.0 / 12.0)
    rate_ref[...] = jnp.broadcast_to(wide[0:1, 0:128], (128, 128)).T[0:sp, :]


def react_kernel(species, dims, odd_ref, hot_ref, count_ref, own_ref, *rest):
    rate_ref, first_ref, second_ref, inner_ref, outer_ref, heat = rest[:6]
    halos, (rea_ref, g_ref, ya_ref, yb_ref, z_ref), (zt,) = rest[6:12], rest[12:17], rest[17:]
    odd = (odd_ref[0], odd_ref[1], odd_ref[2])
    sp = rea_ref.shape[1]

    def store(c, s, n, value):
        rea_ref[c, s : s + n, :] = value

    transport(own_ref, store, species, dims, odd, halos, rate_ref, inner_ref, outer_ref, zt)
    row = lax.broadcasted_iota(jnp.int32, (sp, 128), 0)
    count = count_ref[0]

    def advance(g, carry):
        slots = [hot_ref[g * GROUP + k] for k in range(GROUP)]
        begin = []
        for c in slots:
            extra = jnp.where(row < species + 3, 1.0, -heat[pl.ds(c, 1), :])
            begin.append(jnp.where(row < species, rea_ref[c].astype(bf16).astype(f32), extra))
        start = jnp.concatenate(begin, axis=1)
        current = start
        for section in range(SECTIONS):
            logits = jnp.dot(first_ref[...], current.astype(bf16), preferred_element_type=f32)
            progress = jnp.exp(logits).astype(bf16)
            moved = jnp.dot(second_ref[...], progress, preferred_element_type=f32)
            current = current + moved[0:sp] / (1.0 + moved[sp : 2 * sp])
        increment = (current - start).astype(bf16).astype(f32)
        for k, c in enumerate(slots):

            @pl.when(g * GROUP + k < count)
            def _(k=k, c=c):
                rea_ref[c] = rea_ref[c] + increment[:, k * 128 : (k + 1) * 128]

        return carry

    lax.fori_loop(0, lax.div(count + GROUP - 1, GROUP), advance, jnp.int32(0))

    def load(c, s, n):
        return rea_ref[c, s : s + n, :]

    pack(load, species, dims, odd[1], g_ref, ya_ref, yb_ref, z_ref)


def finish_kernel(species, dims, odd_ref, rea_ref, rate_ref, inner_ref, outer_ref, *rest):
    halos, out_ref, zt = rest[:6], rest[6], rest[7]
    total = dims[0] * dims[1]

    def store(c, s, n, value):
        out_ref[pl.ds(s * total + c, n, stride=total), :] = value

    odd = (odd_ref[0], odd_ref[1], odd_ref[2])
    transport(rea_ref, store, species, dims, odd, halos, rate_ref, inner_ref, outer_ref, zt)


def exchange(packed):
    g, ya, yb, z = packed
    return (
        swap(g, "gx", 0),
        swap(g, "gx", 1),
        swap(ya, "gy", 0),
        swap(yb, "gy", 1),
        swap(z, "gz", 0),
        swap(z, "gz", 1),
    )


def call(kernel, name, outs, in_specs, scratch=()):
    return pl.pallas_call(
        kernel,
        name=name,
        out_shape=outs,
        in_specs=in_specs,
        out_specs=jax.tree.map(lambda _: VMEM, outs),
        scratch_shapes=scratch,
        compiler_params=pltpu.CompilerParams(vmem_limit_bytes=32 << 20),
    )


def body(composition, inv_temp, diffusivity, reactant_orders, net_stoich, log_rate, activation, hot_blocks, hot_counts):
    species, cx, cy, cz = composition.shape
    reactions = reactant_orders.shape[0]
    total, dims = cx * cy, (cx, cy)
    sp, rp = ceil_to(species + 6, 16), ceil_to(reactions, 16)
    shape = jax.ShapeDtypeStruct
    odd = jnp.stack(parities()).astype(jnp.int32)
    field = shape((total, sp, cz), f32)
    packed_out = [shape((total, species, cz), bf16)] + [shape((2 * cx, species, cz), bf16)] * 2 + [shape((species, cz), bf16)]
    own, *packed = call(functools.partial(pack_kernel, species, dims), "pack", [field] + packed_out, [SMEM, VMEM])(
        odd, composition.reshape(species * total, cz)
    )
    table = call(
        functools.partial(prepare_kernel, species, reactions, total),
        "prepare",
        [
            shape((rp, sp), bf16),
            shape((2 * sp, rp), bf16),
            shape((sp, cz), f32),
            shape((256, cz), bf16),
            shape((128, total * cz), bf16),
            shape((total, cz), f32),
        ],
        [ANY] * 6,
        [
            pltpu.VMEM((512, 128), f32),
            pltpu.VMEM((128, 512), f32),
            pltpu.VMEM((reactions, species), bf16),
            pltpu.VMEM((reactions, species), bf16),
            pltpu.VMEM((1, reactions), f32),
            pltpu.VMEM((1, reactions), f32),
            pltpu.VMEM((1, species), f32),
            pltpu.VMEM((total, cz), bf16),
            pltpu.SemaphoreType.DMA((6,)),
        ],
    )(
        reactant_orders,
        net_stoich.T,
        log_rate.reshape(1, -1),
        activation.reshape(1, -1),
        diffusivity.reshape(1, -1),
        inv_temp.reshape(total, cz),
    )
    first, second, rate, inner, outer, heat = table
    scratch = [pltpu.VMEM((total, sp, cz), f32)]
    halos = exchange(packed)
    reacted, *packed = call(
        functools.partial(react_kernel, species, dims), "react", [field] + packed_out, [SMEM] * 3 + [VMEM] * 13, scratch
    )(odd, hot_blocks.reshape(-1), hot_counts.reshape(-1), own, rate, first, second, inner, outer, heat, *halos)
    halos = exchange(packed)
    out = call(
        functools.partial(finish_kernel, species, dims),
        "finish",
        shape((species * total, cz), f32),
        [SMEM] + [VMEM] * 10,
        scratch,
    )(odd, reacted, rate, inner, outer, *halos)
    return out.reshape(composition.shape)


def solution(mesh):
    in_specs = (
        P(None, "gx", "gy", "gz"),
        P("gx", "gy", "gz"),
        P(),
        P(),
        P(),
        P(),
        P(),
        P("gx", "gy", "gz", None),
        P("gx", "gy", "gz"),
    )
    return jax.shard_map(body, mesh=mesh, in_specs=in_specs, out_specs=P(None, "gx", "gy", "gz"), check_vma=False)
```

```python
import functools

import jax
import jax.numpy as jnp
from jax import lax
from jax.experimental import pallas as pl
from jax.experimental.pallas import tpu as pltpu
from jax.sharding import PartitionSpec as P


SECTIONS = 4
ORDERS = (
    ("gx1", "gx0", "gy1", "gz1", "gz0", "gy0"),
    ("gx1", "gx0", "gy1", "gz1", "gz0", "gy0"),
)
GROUP = 4

f32, bf16 = jnp.float32, jnp.bfloat16
VMEM = pl.BlockSpec(memory_space=pltpu.VMEM)
HBM = pl.BlockSpec(memory_space=pltpu.HBM)
SMEM = pl.BlockSpec(memory_space=pltpu.SMEM)


def ceil_to(n, k):
    return -(-n // k) * k


def swap(x, axis, phase):
    n = lax.axis_size(axis)
    pairs = []
    for i in range(phase, n, 2):
        j = (i + 1) % n
        pairs += [(i, j), (j, i)]
    return lax.ppermute(x, axis, pairs)


def chunks(species):
    return [(s, min(16, species - s)) for s in range(0, species, 16)]


def lane_of(rows):
    return lax.broadcasted_iota(jnp.int32, (rows, 128), 1)


def pick(flag, rows):
    return jnp.full((rows, 128), flag, jnp.int32) == 0


def pack(load, species, dims, odd_y, g_ref, ya_ref, yb_ref, z_ref):
    cx, cy = dims
    for s, n in chunks(species):
        lane = lane_of(n)
        even_y = pick(odd_y, n)
        edges = jnp.zeros((n, 128), f32)
        columns = []
        for c in range(cx * cy):
            v = load(c, s, n)
            columns.append(v)
            g_ref[c, s : s + n, :] = v.astype(bf16)
            edges = jnp.where((lane >> 1) == c, pltpu.roll(v, 2 * c, 1) if c else v, edges)
            edges = jnp.where((lane >> 1) == 32 + c, pltpu.roll(v, 2 * c + 66, 1), edges)
        for x in range(cx):
            for k in range(2):
                under, over = columns[x * cy + k], columns[x * cy + cy - 2 + k]
                ya_ref[x * 2 + k, s : s + n, :] = jnp.where(even_y, over, under).astype(bf16)
                yb_ref[x * 2 + k, s : s + n, :] = jnp.where(even_y, under, over).astype(bf16)
        z_ref[s : s + n, :] = edges.astype(bf16)


def stencil_of(distance):
    reach = jnp.abs(distance)
    w = jnp.where(reach == 1, 16.0, jnp.where(reach == 2, -1.0, 0.0))
    return jnp.where(reach == 0, -90.0, w)


def transport(own_ref, store, species, dims, odd, halos, rate_ref, inner_ref, outer_ref, zt, after=None):
    cx, cy = dims
    total = cx * cy
    odd_x, odd_y, odd_z = odd
    ga_ref, gb_ref, ya_ref, yb_ref, za_ref, zb_ref = halos
    sp = own_ref.shape[1]
    v = own_ref[...].reshape(total * sp, 128)
    high = v.astype(bf16)
    low = (v - high.astype(f32)).astype(bf16)
    zt[...] = jnp.dot(jnp.concatenate([high, low], axis=1), inner_ref[...], preferred_element_type=f32).reshape(total, sp, 128)
    even_z = (lane_of(species) < 64) == pick(odd_z, species)
    edges = jnp.where(even_z, za_ref[...].astype(f32), zb_ref[...].astype(f32)).astype(bf16)
    rim = jnp.dot(edges, outer_ref[...], preferred_element_type=f32)
    for c in range(total):
        zt[c, 0:species, :] = zt[c, 0:species, :] + rim[:, c * 128 : c * 128 + 128]
    for s, n in chunks(species):
        even_x, even_y = pick(odd_x, n), pick(odd_y, n)

        def both(a, b, even):
            a, b = a.astype(f32), b.astype(f32)
            return jnp.where(even, a, b), jnp.where(even, b, a)

        rows = slice(s, s + n)
        rate = rate_ref[rows, :]
        v = [own_ref[c, rows, :] for c in range(total)]
        up, down = [], []
        for k in range(2 * cx):
            above, under = both(ya_ref[k, rows, :], yb_ref[k, rows, :], even_y)
            up.append(above)
            down.append(under)
        for y in range(cy):
            right0, left0 = both(ga_ref[y, rows, :], gb_ref[y, rows, :], even_x)
            right1, left1 = both(ga_ref[cy + y, rows, :], gb_ref[cy + y, rows, :], even_x)
            line = [left0, left1, v[y], v[cy + y], right0, right1]
            for x in range(cx):
                c = x * cy + y
                ys = down[2 * x : 2 * x + 2] + v[x * cy : x * cy + cy] + up[2 * x : 2 * x + 2]
                near = (line[x + 1] + line[x + 3]) + (ys[y + 1] + ys[y + 3])
                far = (line[x] + line[x + 4]) + (ys[y] + ys[y + 4])
                store(c, s, n, v[c] + rate * (16.0 * near - far + zt[c, rows, :]))
        if after is not None:
            after(s, n)


def parities():
    return tuple(lax.rem(lax.axis_index(a), 2) for a in ("gx", "gy", "gz"))


def pack_kernel(species, dims, comp_hbm, *refs):
    sources, own_ref, outs, targets = refs[:6], refs[6], refs[7:11], refs[11:17]
    comp, sems, param_sems = refs[17:]
    total = dims[0] * dims[1]
    parts = []
    for k, (s, n) in enumerate(chunks(species)):
        rows = pl.ds(s * total, n * total)
        parts.append(pltpu.make_async_copy(comp_hbm.at[rows, :], comp.at[rows, :], sems.at[k]))
        parts[-1].start()
    moves = [pltpu.make_async_copy(a, b, param_sems.at[k]) for k, (a, b) in enumerate(zip(sources, targets))]
    for move in moves:
        move.start()
    odd_y = parities()[1]

    def load(c, s, n):
        if c == 0:
            parts[s // 16].wait()
        value = comp[pl.ds(s * total + c, n, stride=total), :]
        own_ref[c, s : s + n, :] = value
        return value

    pack(load, species, dims, odd_y, *outs)
    for move in moves:
        move.wait()


def prepare_kernel(species, reactions, columns, *refs):
    orders, net, log, act, diff, heat = refs[:6]
    first_ref, second_ref, rate_ref, inner_ref, outer_ref, heat_ref = refs[6:12]
    tall, wide = refs[12:]
    k, lane = lax.broadcasted_iota(jnp.int32, (128, 128), 0), lane_of(128)
    inner = stencil_of(lane - k).astype(bf16)
    inner_ref[0:128, :] = inner
    inner_ref[128:256, :] = inner
    outer = stencil_of(lane - (jnp.where(k < 64, 128, -2) + (k & 1)))
    for c in range(columns):
        outer_ref[:, c * 128 : c * 128 + 128] = jnp.where(((k & 63) >> 1) == c, outer, 0.0).astype(bf16)
    wide[...] = jnp.zeros_like(wide)
    tall[...] = jnp.zeros_like(tall)
    heat_ref[...] = heat[...].astype(f32)
    rp, sp = first_ref.shape
    for row, ref in ((species, log), (species + 3, act)):
        rest = ref[...]
        for k in range(3):
            part = rest.astype(bf16).astype(f32)
            wide[row + k : row + k + 1, 0:reactions] = part
            rest = rest - part
    tall[0:reactions, 0:species] = orders[...].astype(f32)
    first_ref[...] = (tall[...] + wide[...].T)[0:rp, 0:sp].astype(bf16)
    second_ref[sp : 2 * sp, :] = (0.5 * tall[...]).T[0:sp, 0:rp].astype(bf16)
    tall[0:reactions, 0:species] = 0.5 * net[...].astype(f32)
    second_ref[0:sp, :] = tall[...].T[0:sp, 0:rp].astype(bf16)
    wide[0:1, 0:species] = diff[...] * (1.0 / 12.0)
    rate_ref[...] = jnp.broadcast_to(wide[0:1, 0:128], (128, 128)).T[0:sp, :]


def react_kernel(species, dims, count_ref, hot_hbm, own_ref, *rest):
    rate_ref, first_ref, second_ref, inner_ref, outer_ref, heat = rest[:6]
    halos, (rea_ref, g_ref, ya_ref, yb_ref, z_ref) = rest[6:12], rest[12:17]
    zt, hot_ref, sem = rest[17:]
    move = pltpu.make_async_copy(hot_hbm, hot_ref, sem)
    move.start()
    odd = parities()
    sp = rea_ref.shape[1]

    def store(c, s, n, value):
        rea_ref[c, s : s + n, :] = value

    transport(own_ref, store, species, dims, odd, halos, rate_ref, inner_ref, outer_ref, zt)
    row = lax.broadcasted_iota(jnp.int32, (sp, 128), 0)
    move.wait()
    count = count_ref[0, 0, 0]

    def advance(g, carry):
        slots = [hot_ref[0, 0, 0, g * GROUP + k] for k in range(GROUP)]
        begin = []
        for c in slots:
            extra = jnp.where(row < species + 3, 1.0, -heat[pl.ds(c, 1), :])
            begin.append(jnp.where(row < species, rea_ref[c].astype(bf16).astype(f32), extra))
        start = jnp.concatenate(begin, axis=1)
        current = start
        for _ in range(SECTIONS):
            logits = jnp.dot(first_ref[...], current.astype(bf16), preferred_element_type=f32)
            progress = jnp.exp(logits).astype(bf16)
            moved = jnp.dot(second_ref[...], progress, preferred_element_type=f32)
            current = current + moved[0:sp] / (1.0 + moved[sp : 2 * sp])
        increment = (current - start).astype(bf16).astype(f32)
        for k, c in enumerate(slots):

            @pl.when(g * GROUP + k < count)
            def _(k=k, c=c):
                rea_ref[c] = rea_ref[c] + increment[:, k * 128 : (k + 1) * 128]

        return carry

    lax.fori_loop(0, lax.div(count + GROUP - 1, GROUP), advance, jnp.int32(0))

    def load(c, s, n):
        return rea_ref[c, s : s + n, :]

    pack(load, species, dims, odd[1], g_ref, ya_ref, yb_ref, z_ref)


def finish_kernel(species, dims, rea_ref, rate_ref, inner_ref, outer_ref, *rest):
    halos, out_hbm, zt, out, sems = rest[:6], rest[6], rest[7], rest[8], rest[9]
    total = dims[0] * dims[1]
    moves = []
    for k, (s, n) in enumerate(chunks(species)):
        rows = pl.ds(s * total, n * total)
        moves.append(pltpu.make_async_copy(out.at[rows, :], out_hbm.at[rows, :], sems.at[k]))

    def store(c, s, n, value):
        out[pl.ds(s * total + c, n, stride=total), :] = value

    def after(s, n):
        if s:
            moves[s // 16 - 1].start()

    transport(rea_ref, store, species, dims, parities(), halos, rate_ref, inner_ref, outer_ref, zt, after)
    moves[-1].start()
    for move in moves:
        move.wait()


def exchange(packed, step):
    g, ya, yb, z = packed
    sent = {"gx0": g, "gx1": g, "gy0": ya, "gy1": yb, "gz0": z, "gz1": z}
    got = {}
    for name in ORDERS[step]:
        got[name] = swap(sent[name], name[:2], int(name[2]))
    return tuple(got[name] for name in sorted(got))


def call(kernel, outs, in_specs, scratch=(), out_spec=VMEM):
    return pl.pallas_call(
        kernel,
        out_shape=outs,
        in_specs=in_specs,
        out_specs=jax.tree.map(lambda _: out_spec, outs),
        scratch_shapes=scratch,
        compiler_params=pltpu.CompilerParams(vmem_limit_bytes=32 << 20),
    )


def body(composition, inv_temp, diffusivity, reactant_orders, net_stoich, log_rate, activation, hot_blocks, hot_counts):
    species, cx, cy, cz = composition.shape
    reactions = reactant_orders.shape[0]
    total, dims = cx * cy, (cx, cy)
    sp, rp = ceil_to(species + 6, 16), ceil_to(reactions, 16)
    shape = jax.ShapeDtypeStruct
    dma = pltpu.SemaphoreType.DMA
    pieces = len(chunks(species))
    field = shape((total, sp, cz), f32)
    packed_out = [shape((total, species, cz), bf16)] + [shape((2 * cx, species, cz), bf16)] * 2 + [shape((species, cz), bf16)]
    params = (
        reactant_orders,
        net_stoich.T,
        log_rate.reshape(1, -1),
        activation.reshape(1, -1),
        diffusivity.reshape(1, -1),
        inv_temp.reshape(total, cz),
    )
    params = tuple(pltpu.with_memory_space_constraint(p, pltpu.HBM) for p in params)
    comp = pltpu.with_memory_space_constraint(composition.reshape(species * total, cz), pltpu.HBM)
    hot_blocks = pltpu.with_memory_space_constraint(hot_blocks, pltpu.HBM)
    own, *rest = call(
        functools.partial(pack_kernel, species, dims),
        [field] + packed_out + [shape(p.shape, p.dtype) for p in params],
        [HBM] * 7,
        [pltpu.VMEM((species * total, cz), f32), dma((pieces,)), dma((6,))],
    )(comp, *params)
    packed, params = rest[:4], rest[4:]
    first, second, rate, inner, outer, heat = call(
        functools.partial(prepare_kernel, species, reactions, total),
        [
            shape((rp, sp), bf16),
            shape((2 * sp, rp), bf16),
            shape((sp, cz), f32),
            shape((256, cz), bf16),
            shape((128, total * cz), bf16),
            shape((total, cz), f32),
        ],
        [VMEM] * 6,
        [pltpu.VMEM((512, 128), f32), pltpu.VMEM((128, 512), f32)],
    )(*params)
    halos = exchange(packed, 0)
    zt = pltpu.VMEM((total, sp, cz), f32)
    reacted, *packed = call(
        functools.partial(react_kernel, species, dims),
        [field] + packed_out,
        [SMEM, HBM] + [VMEM] * 13,
        [zt, pltpu.SMEM(hot_blocks.shape, jnp.int32), dma],
    )(hot_counts, hot_blocks, own, rate, first, second, inner, outer, heat, *halos)
    halos = exchange(packed, 1)
    out = call(
        functools.partial(finish_kernel, species, dims),
        shape((species * total, cz), f32),
        [VMEM] * 10,
        [zt, pltpu.VMEM((species * total, cz), f32), dma((pieces,))],
        HBM,
    )(reacted, rate, inner, outer, *halos)
    return out.reshape(composition.shape)


def solution(mesh):
    in_specs = (
        P(None, "gx", "gy", "gz"),
        P("gx", "gy", "gz"),
        P(),
        P(),
        P(),
        P(),
        P(),
        P("gx", "gy", "gz", None),
        P("gx", "gy", "gz"),
    )
    return jax.shard_map(body, mesh=mesh, in_specs=in_specs, out_specs=P(None, "gx", "gy", "gz"), check_vma=False)
```

```python
import functools

import jax
import jax.numpy as jnp
from jax import lax
from jax.experimental import pallas as pl
from jax.experimental.pallas import tpu as pltpu
from jax.sharding import PartitionSpec as P


SECTIONS = 4
ORDERS = (
    ("gx1", "gy1", "gx0", "gz1", "gz0", "gy0"),
    ("gx1", "gy1", "gx0", "gz1", "gz0", "gy0"),
)
GROUP = 8

f32, bf16 = jnp.float32, jnp.bfloat16
VMEM = pl.BlockSpec(memory_space=pltpu.VMEM)
HBM = pl.BlockSpec(memory_space=pltpu.HBM)
SMEM = pl.BlockSpec(memory_space=pltpu.SMEM)


def ceil_to(n, k):
    return -(-n // k) * k


def swap(x, axis, phase):
    n = lax.axis_size(axis)
    pairs = []
    for i in range(phase, n, 2):
        j = (i + 1) % n
        pairs += [(i, j), (j, i)]
    return lax.ppermute(x, axis, pairs)


def chunks(species):
    return [(s, min(16, species - s)) for s in range(0, species, 16)]


def lane_of(rows):
    return lax.broadcasted_iota(jnp.int32, (rows, 128), 1)


def pick(flag, rows):
    return jnp.full((rows, 128), flag, jnp.int32) == 0


def pack(load, species, dims, odd_y, g_ref, ya_ref, yb_ref, z_ref):
    cx, cy = dims
    for s, n in chunks(species):
        lane = lane_of(n)
        even_y = pick(odd_y, n)
        edges = jnp.zeros((n, 128), f32)
        columns = []
        for c in range(cx * cy):
            v = load(c, s, n)
            columns.append(v)
            g_ref[c, s : s + n, :] = v.astype(bf16)
            edges = jnp.where((lane >> 1) == c, pltpu.roll(v, 2 * c, 1) if c else v, edges)
            edges = jnp.where((lane >> 1) == 32 + c, pltpu.roll(v, 2 * c + 66, 1), edges)
        for x in range(cx):
            for k in range(2):
                under, over = columns[x * cy + k], columns[x * cy + cy - 2 + k]
                ya_ref[x * 2 + k, s : s + n, :] = jnp.where(even_y, over, under).astype(bf16)
                yb_ref[x * 2 + k, s : s + n, :] = jnp.where(even_y, under, over).astype(bf16)
        z_ref[s : s + n, :] = edges.astype(bf16)


def stencil_of(distance):
    reach = jnp.abs(distance)
    w = jnp.where(reach == 1, 16.0, jnp.where(reach == 2, -1.0, 0.0))
    return jnp.where(reach == 0, -90.0, w)


def along_z(own_ref, inner_ref, zt):
    total, sp, _ = own_ref.shape
    v = own_ref[...].reshape(total * sp, 128)
    high = v.astype(bf16)
    low = (v - high.astype(f32)).astype(bf16)
    zt[...] = jnp.dot(jnp.concatenate([high, low], axis=1), inner_ref[...], preferred_element_type=f32).reshape(total, sp, 128)


def transport(own_ref, store, species, dims, odd, halos, rate_ref, inner_ref, outer_ref, zt, after=None, ready=None):
    cx, cy = dims
    total = cx * cy
    odd_x, odd_y, odd_z = odd
    ga_ref, gb_ref, ya_ref, yb_ref, za_ref, zb_ref = halos
    if ready is None:
        along_z(own_ref, inner_ref, zt)
        ready = zt
    even_z = (lane_of(species) < 64) == pick(odd_z, species)
    edges = jnp.where(even_z, za_ref[...].astype(f32), zb_ref[...].astype(f32)).astype(bf16)
    rim = jnp.dot(edges, outer_ref[...], preferred_element_type=f32)
    for c in range(total):
        zt[c, 0:species, :] = ready[c, 0:species, :] + rim[:, c * 128 : c * 128 + 128]
    for s, n in chunks(species):
        even_x, even_y = pick(odd_x, n), pick(odd_y, n)

        def both(a, b, even):
            a, b = a.astype(f32), b.astype(f32)
            return jnp.where(even, a, b), jnp.where(even, b, a)

        rows = slice(s, s + n)
        rate = rate_ref[rows, :]
        v = [own_ref[c, rows, :] for c in range(total)]
        up, down = [], []
        for k in range(2 * cx):
            above, under = both(ya_ref[k, rows, :], yb_ref[k, rows, :], even_y)
            up.append(above)
            down.append(under)
        for y in range(cy):
            right0, left0 = both(ga_ref[y, rows, :], gb_ref[y, rows, :], even_x)
            right1, left1 = both(ga_ref[cy + y, rows, :], gb_ref[cy + y, rows, :], even_x)
            line = [left0, left1, v[y], v[cy + y], right0, right1]
            for x in range(cx):
                c = x * cy + y
                ys = down[2 * x : 2 * x + 2] + v[x * cy : x * cy + cy] + up[2 * x : 2 * x + 2]
                near = (line[x + 1] + line[x + 3]) + (ys[y + 1] + ys[y + 3])
                far = (line[x] + line[x + 4]) + (ys[y] + ys[y + 4])
                store(c, s, n, v[c] + rate * (16.0 * near - far + zt[c, rows, :]))
        if after is not None:
            after(s, n)


def parities():
    return tuple(lax.rem(lax.axis_index(a), 2) for a in ("gx", "gy", "gz"))


def pack_kernel(species, dims, comp_hbm, *refs):
    sources, own_ref, outs, targets = refs[:6], refs[6], refs[7:11], refs[11:17]
    comp, sems, param_sems = refs[17:]
    total = dims[0] * dims[1]
    parts = []
    for k, (s, n) in enumerate(chunks(species)):
        rows = pl.ds(s * total, n * total)
        parts.append(pltpu.make_async_copy(comp_hbm.at[rows, :], comp.at[rows, :], sems.at[k]))
        parts[-1].start()
    moves = [pltpu.make_async_copy(a, b, param_sems.at[k]) for k, (a, b) in enumerate(zip(sources, targets))]
    for move in moves:
        move.start()
    odd_y = parities()[1]

    for part in parts:
        part.wait()

    def load(c, s, n):
        value = comp[pl.ds(s * total + c, n, stride=total), :]
        own_ref[c, s : s + n, :] = value
        return value

    pack(load, species, dims, odd_y, *outs)
    for move in moves:
        move.wait()


def prepare_kernel(species, reactions, columns, *refs):
    orders, net, log, act, diff, heat = refs[:6]
    first_ref, second_ref, rate_ref, inner_ref, outer_ref, heat_ref = refs[6:12]
    tall, wide = refs[12:]
    k, lane = lax.broadcasted_iota(jnp.int32, (128, 128), 0), lane_of(128)
    inner = stencil_of(lane - k).astype(bf16)
    inner_ref[0:128, :] = inner
    inner_ref[128:256, :] = inner
    outer = stencil_of(lane - (jnp.where(k < 64, 128, -2) + (k & 1)))
    for c in range(columns):
        outer_ref[:, c * 128 : c * 128 + 128] = jnp.where(((k & 63) >> 1) == c, outer, 0.0).astype(bf16)
    wide[...] = jnp.zeros_like(wide)
    tall[...] = jnp.zeros_like(tall)
    heat_ref[...] = heat[...].astype(f32)
    rp, sp = first_ref.shape
    for row, ref in ((species, log), (species + 3, act)):
        rest = ref[...]
        for k in range(3):
            part = rest.astype(bf16).astype(f32)
            wide[row + k : row + k + 1, 0:reactions] = part
            rest = rest - part
    tall[0:reactions, 0:species] = orders[...].astype(f32)
    first_ref[...] = (tall[...] + wide[...].T)[0:rp, 0:sp].astype(bf16)
    second_ref[sp : 2 * sp, :] = (0.5 * tall[...]).T[0:sp, 0:rp].astype(bf16)
    tall[0:reactions, 0:species] = 0.5 * net[...].astype(f32)
    second_ref[0:sp, :] = tall[...].T[0:sp, 0:rp].astype(bf16)
    wide[0:1, 0:species] = diff[...] * (1.0 / 12.0)
    rate_ref[...] = jnp.broadcast_to(wide[0:1, 0:128], (128, 128)).T[0:sp, :]


def react_kernel(species, dims, count_ref, hot_hbm, own_ref, *rest):
    rate_ref, first_ref, second_ref, inner_ref, outer_ref, heat = rest[:6]
    halos, (rea_ref, g_ref, ya_ref, yb_ref, z_ref) = rest[6:12], rest[12:17]
    zt, hot_ref, sem = rest[17:]
    move = pltpu.make_async_copy(hot_hbm, hot_ref, sem)
    move.start()
    odd = parities()
    sp = rea_ref.shape[1]

    def store(c, s, n, value):
        rea_ref[c, s : s + n, :] = value

    transport(own_ref, store, species, dims, odd, halos, rate_ref, inner_ref, outer_ref, zt)
    row = lax.broadcasted_iota(jnp.int32, (sp, 128), 0)
    move.wait()
    count = count_ref[0, 0, 0]

    def advance(g, carry):
        slots = [hot_ref[0, 0, 0, g * GROUP + k] for k in range(GROUP)]
        begin = []
        for c in slots:
            extra = jnp.where(row < species + 3, 1.0, -heat[pl.ds(c, 1), :])
            begin.append(jnp.where(row < species, rea_ref[c].astype(bf16).astype(f32), extra))
        start = jnp.concatenate(begin, axis=1)
        current = start
        for _ in range(SECTIONS):
            logits = jnp.dot(first_ref[...], current.astype(bf16), preferred_element_type=f32)
            progress = jnp.exp(logits).astype(bf16)
            moved = jnp.dot(second_ref[...], progress, preferred_element_type=f32)
            current = current + moved[0:sp] / (1.0 + moved[sp : 2 * sp])
        increment = (current - start).astype(bf16).astype(f32)
        for k, c in enumerate(slots):

            @pl.when(g * GROUP + k < count)
            def _(k=k, c=c):
                rea_ref[c] = rea_ref[c] + increment[:, k * 128 : (k + 1) * 128]

        return carry

    lax.fori_loop(0, lax.div(count + GROUP - 1, GROUP), advance, jnp.int32(0))

    def load(c, s, n):
        return rea_ref[c, s : s + n, :]

    pack(load, species, dims, odd[1], g_ref, ya_ref, yb_ref, z_ref)


def finish_kernel(species, dims, rea_ref, rate_ref, ready, outer_ref, *rest):
    halos, out_hbm, zt, out, sems = rest[:6], rest[6], rest[7], rest[8], rest[9]
    total = dims[0] * dims[1]
    moves = []
    for k, (s, n) in enumerate(chunks(species)):
        rows = pl.ds(s * total, n * total)
        moves.append(pltpu.make_async_copy(out.at[rows, :], out_hbm.at[rows, :], sems.at[k]))

    def store(c, s, n, value):
        out[pl.ds(s * total + c, n, stride=total), :] = value

    def after(s, n):
        if s:
            moves[s // 16 - 1].start()

    transport(rea_ref, store, species, dims, parities(), halos, rate_ref, None, outer_ref, zt, after, ready)
    moves[-1].start()
    for move in moves:
        move.wait()


def exchange(packed, step):
    g, ya, yb, z = packed
    sent = {"gx0": g, "gx1": g, "gy0": ya, "gy1": yb, "gz0": z, "gz1": z}
    got = {}
    for name in ORDERS[step]:
        got[name] = swap(sent[name], name[:2], int(name[2]))
    return tuple(got[name] for name in sorted(got))


def call(kernel, outs, in_specs, scratch=(), out_spec=VMEM):
    return pl.pallas_call(
        kernel,
        out_shape=outs,
        in_specs=in_specs,
        out_specs=jax.tree.map(lambda _: out_spec, outs),
        scratch_shapes=scratch,
        compiler_params=pltpu.CompilerParams(vmem_limit_bytes=32 << 20),
    )


def body(composition, inv_temp, diffusivity, reactant_orders, net_stoich, log_rate, activation, hot_blocks, hot_counts):
    species, cx, cy, cz = composition.shape
    reactions = reactant_orders.shape[0]
    total, dims = cx * cy, (cx, cy)
    sp, rp = ceil_to(species + 6, 16), ceil_to(reactions, 16)
    shape = jax.ShapeDtypeStruct
    dma = pltpu.SemaphoreType.DMA
    pieces = len(chunks(species))
    field = shape((total, sp, cz), f32)
    packed_out = [shape((total, species, cz), bf16)] + [shape((2 * cx, species, cz), bf16)] * 2 + [shape((species, cz), bf16)]
    params = (
        reactant_orders,
        net_stoich.T,
        log_rate.reshape(1, -1),
        activation.reshape(1, -1),
        diffusivity.reshape(1, -1),
        inv_temp.reshape(total, cz),
    )
    params = tuple(pltpu.with_memory_space_constraint(p, pltpu.HBM) for p in params)
    comp = pltpu.with_memory_space_constraint(composition.reshape(species * total, cz), pltpu.HBM)
    hot_blocks = pltpu.with_memory_space_constraint(hot_blocks, pltpu.HBM)
    own, *rest = call(
        functools.partial(pack_kernel, species, dims),
        [field] + packed_out + [shape(p.shape, p.dtype) for p in params],
        [HBM] * 7,
        [pltpu.VMEM((species * total, cz), f32), dma((pieces,)), dma((6,))],
    )(comp, *params)
    packed, params = rest[:4], rest[4:]
    first, second, rate, inner, outer, heat = call(
        functools.partial(prepare_kernel, species, reactions, total),
        [
            shape((rp, sp), bf16),
            shape((2 * sp, rp), bf16),
            shape((sp, cz), f32),
            shape((256, cz), bf16),
            shape((128, total * cz), bf16),
            shape((total, cz), f32),
        ],
        [VMEM] * 6,
        [pltpu.VMEM((512, 128), f32), pltpu.VMEM((128, 512), f32)],
    )(*params)
    halos = exchange(packed, 0)
    zt = pltpu.VMEM((total, sp, cz), f32)
    reacted, *packed = call(
        functools.partial(react_kernel, species, dims),
        [field] + packed_out,
        [SMEM, HBM] + [VMEM] * 13,
        [zt, pltpu.SMEM(hot_blocks.shape, jnp.int32), dma],
    )(hot_counts, hot_blocks, own, rate, first, second, inner, outer, heat, *halos)
    ready = call(along_z, field, [VMEM] * 2)(reacted, inner)
    halos = exchange(packed, 1)
    out = call(
        functools.partial(finish_kernel, species, dims),
        shape((species * total, cz), f32),
        [VMEM] * 10,
        [zt, pltpu.VMEM((species * total, cz), f32), dma((pieces,))],
        HBM,
    )(reacted, rate, ready, outer, *halos)
    return out.reshape(composition.shape)


def solution(mesh):
    in_specs = (
        P(None, "gx", "gy", "gz"),
        P("gx", "gy", "gz"),
        P(),
        P(),
        P(),
        P(),
        P(),
        P("gx", "gy", "gz", None),
        P("gx", "gy", "gz"),
    )
    return jax.shard_map(body, mesh=mesh, in_specs=in_specs, out_specs=P(None, "gx", "gy", "gz"), check_vma=False)
```
